256 devices in a mesh: gx: 4 (over x), gy: 8 (over z_lo, core), gz: 8 (over y, z_hi).
Axes of the slice: x: 4, y: 4, z: 8 (z_hi: 2, z_lo: 4; z = z_hi * 4 + z_lo), core: 2. Of those that a mesh axis runs over, the one named last changes fastest.
Arguments:
- energy: float32 [256, 256, 1024], P(('gz', 'gy', 'gx')), may hold values from -5 to 5
- flow: float32 [4, 256, 256, 1024], P(None, ('gz', 'gy', 'gx')), may hold values from -0.1 to 0.12, as said below
Outputs:
- energy_next: float32 [256, 256, 1024], P('gz', 'gx', 'gy')
- plane_mean: float32 [256], P('gz')
- running_mean: float32 [256], P('gz')
The draws below stay inside these ranges and needn't reach their ends.
Inputs may be any that keep to these rules, and one draw needn't show every extreme that they name: flow[0], flow[1] and flow[2] lie within -0.1 to 0.1; flow[3] lies within 0.02 to 0.12.
All inputs are finite; a program needn't handle non-finite values.
Results may differ from the reference program's by a relative error of at most 0.00002.
Values sent between devices are 32-bit elements; how exact they have to be, the bound alone decides.
No kernel may reach another device: no remote copies, remote signals or barrier semaphores. Data moves between devices by JAX's collectives and lax.ppermute only.
A program may use at most 128 MiB of HBM per device.

```python
import math
import jax
import jax.numpy as jnp

NX = 256
NY = 1024
NZ = 256


def draw_energy(key, part):
    noise_key, phase_key, offset_key = jax.random.split(jax.random.fold_in(key, 11), 3)
    phases = jax.random.uniform(phase_key, (3,), jnp.float32, 0.0, 2.0 * math.pi)
    z_fraction = (jnp.arange(NZ, dtype=jnp.float32) / NZ)[:, None, None]
    x_fraction = (jnp.arange(NX, dtype=jnp.float32) / NX)[None, :, None]
    y_fraction = (jnp.arange(NY, dtype=jnp.float32) / NY)[None, None, :]
    offsets = jax.random.uniform(offset_key, (NZ, 1, 1), jnp.float32, -1.2, 1.2)
    smooth = offsets + 0.6 * jnp.sin(2.0 * math.pi * x_fraction + phases[0]) * jnp.cos(2.0 * math.pi * z_fraction + phases[1]) + 0.3 * jnp.cos(2.0 * math.pi * y_fraction + phases[2])
    noise = 0.8 * jnp.clip(jax.random.normal(noise_key, (NZ, NX, NY), jnp.float32), -3.0, 3.0)
    return (smooth + noise).astype(jnp.float32)


def draw_flow(key, part):
    speed_key, kappa_key = jax.random.split(jax.random.fold_in(key, 23))
    speeds = jax.random.uniform(speed_key, (3, NZ, NX, NY), jnp.float32, -0.1, 0.1)
    conductivity = jnp.exp(jax.random.uniform(kappa_key, (1, NZ, NX, NY), jnp.float32, math.log(0.02), math.log(0.12)))
    return jnp.concatenate([speeds, conductivity], 0).astype(jnp.float32)


def setup_inputs(seed: int = 0) -> dict:
    seeds = jax.random.split(jax.random.key(seed), 3)
    return {
        "energy": draw_energy(jax.random.fold_in(seeds[2], 71), 0),
        "flow": draw_flow(jax.random.fold_in(seeds[2], 71), 0),
    }


directions = ((1, 0, 0), (0, 1, 0), (0, 0, 1))


def extend(field):
    padded = jnp.pad(field, ((0, 0), (1, 1), (1, 1)))
    return jnp.concatenate([padded[-1:], padded, padded[:1]], 0)


def window(array, offset):
    return array[1 + offset[0]: array.shape[0] - 1 + offset[0],
                 1 + offset[1]: array.shape[1] - 1 + offset[1],
                 1 + offset[2]: array.shape[2] - 1 + offset[2]]


def advance(energy_pad, kappa_pad, velocity):
    centre = window(energy_pad, (0, 0, 0))
    kappa_centre = window(kappa_pad, (0, 0, 0))
    change = jnp.zeros_like(centre)
    for axis_number, forward in enumerate(directions):
        backward = tuple(-item for item in forward)
        upper = window(energy_pad, forward)
        lower = window(energy_pad, backward)
        kappa_upper = window(kappa_pad, forward)
        kappa_lower = window(kappa_pad, backward)
        change = change + 0.5 * (kappa_centre + kappa_upper) * (upper - centre) - 0.5 * (kappa_centre + kappa_lower) * (centre - lower)
        speed = velocity[axis_number]
        change = change - jnp.maximum(speed, 0.0) * (centre - lower) - jnp.minimum(speed, 0.0) * (upper - centre)
    return centre + change


def reference(energy, flow):
    velocity = flow[:3]
    kappa_pad = extend(flow[3])
    energy_half = advance(extend(energy), kappa_pad, velocity)
    energy_next = advance(extend(energy_half), kappa_pad, velocity)
    plane_mean = jnp.sum(energy_next, axis=(1, 2)) / (NX * NY)
    ranks = jnp.arange(1, NZ + 1).astype(jnp.float32)
    running_mean = jnp.cumsum(plane_mean) / ranks
    return energy_next, plane_mean, running_mean
```

```python
import functools

import jax
import jax.numpy as jnp
from jax import lax
from jax.experimental import pallas as pl
from jax.experimental.pallas import tpu as pltpu
from jax.sharding import PartitionSpec as P

F32 = jnp.float32
ANY = pl.BlockSpec(memory_space=pl.ANY)
SMEM = pl.BlockSpec(memory_space=pltpu.SMEM)
VMEM = pl.BlockSpec(memory_space=pltpu.VMEM)
LANES = 128
ROWS = 8
EDGE = 2 * ROWS


def params(mib=48):
    return pltpu.CompilerParams(vmem_limit_bytes=mib * 2**20)


def rows_of(shape):
    return lax.broadcasted_iota(jnp.int32, shape, 0)


def lanes_of(shape):
    return lax.broadcasted_iota(jnp.int32, shape, 1)


def down(tile, count):
    count %= ROWS
    return pltpu.roll(tile, count, 0) if count else tile


def pack_body(parts, rows, slots, idx, energy, flow, *refs):
    outs, (low, high, edges, sem, tile_sem) = refs[: 2 * len(slots)], refs[2 * len(slots) :]
    me = idx[0]
    fields = [energy.at[0]] + [flow.at[c, 0] for c in (3, 0, 1, 2)]
    copies, tiles = [], []
    for n, slot in enumerate(slots):
        to = lax.rem(me + slot, parts)
        first = pl.multiple_of(to * rows, ROWS)
        before = pl.multiple_of(jnp.maximum(first - ROWS, 0), ROWS)
        after = pl.multiple_of(jnp.minimum(first + rows, (parts * rows) - ROWS), ROWS)
        for f, field in enumerate(fields):
            for at, held in ((before, low), (after, high)):
                tiles.append(
                    pltpu.make_async_copy(field.at[pl.ds(at, ROWS)], held.at[n, f], tile_sem)
                )
    for copy in tiles:
        copy.start()
    for n, slot in enumerate(slots):
        to = lax.rem(me + slot, parts)
        first = pl.multiple_of(to * rows, ROWS)
        for f, field in enumerate(fields):
            out, at = (outs[2 * n], f * rows) if f < 2 else (outs[2 * n + 1], (f - 2) * rows)
            copies.append(
                pltpu.make_async_copy(field.at[pl.ds(first, rows)], out.at[pl.ds(at, rows)], sem)
            )
    for copy in copies:
        copy.start()
    for copy in tiles:
        copy.wait()
    for n, slot in enumerate(slots):
        to = lax.rem(me + slot, parts)
        row = rows_of(low.shape[2:])
        top, bottom = jnp.zeros(low.shape[2:], F32), jnp.zeros(low.shape[2:], F32)
        for f, (begin, count) in enumerate(((0, 2), (2, 2), (4, 1), (5, 1), (6, 1))):
            here = (row >= begin) & (row < begin + count)
            top = jnp.where(here, down(low[n, f], begin + count), top)
            bottom = jnp.where(here, down(high[n, f], begin), bottom)
        edges[n, :ROWS] = jnp.where(to == 0, 0.0, top)
        edges[n, ROWS:] = jnp.where(to == parts - 1, 0.0, bottom)
    for n, _ in enumerate(slots):
        copy = pltpu.make_async_copy(edges.at[n], outs[2 * n].at[pl.ds(2 * rows, EDGE)], sem)
        copy.start()
        copies.append(copy)
    for copy in copies:
        copy.wait()


def pack(idx, energy, flow, parts, slots):
    rows, width = energy.shape[1] // parts, energy.shape[2]
    shapes = [
        jax.ShapeDtypeStruct((2 * rows + EDGE, width), F32),
        jax.ShapeDtypeStruct((3 * rows, width), F32),
    ] * len(slots)
    out = pl.pallas_call(
        functools.partial(pack_body, parts, rows, slots),
        out_shape=shapes,
        in_specs=[SMEM, ANY, ANY],
        out_specs=[ANY] * len(shapes),
        scratch_shapes=[
            pltpu.VMEM((len(slots), 5, ROWS, width), F32),
            pltpu.VMEM((len(slots), 5, ROWS, width), F32),
            pltpu.VMEM((len(slots), EDGE, width), F32),
            pltpu.SemaphoreType.DMA,
            pltpu.SemaphoreType.DMA,
        ],
        compiler_params=params(),
        name="pack",
    )(idx, energy, flow)
    return list(zip(out[0::2], out[1::2]))


def ends_body(parts, idx, *refs):
    slots, lowest, highest, sem = refs[:parts], *refs[parts:]
    me = idx[0]
    for slot, ref in enumerate(slots):
        plane = lax.rem(me - slot + parts, parts)
        for wanted, out in ((0, lowest), (parts - 1, highest)):

            @pl.when(plane == wanted)
            def _():
                pltpu.make_async_copy(ref, out, sem).start()

    for out in (lowest, highest):
        pltpu.make_async_copy(slots[0], out, sem).wait()


def ends(idx, slots):
    shape = jax.ShapeDtypeStruct(slots[0].shape, F32)
    return pl.pallas_call(
        functools.partial(ends_body, len(slots)),
        out_shape=[shape] * 2,
        in_specs=[SMEM] + [ANY] * len(slots),
        out_specs=[ANY] * 2,
        scratch_shapes=[pltpu.SemaphoreType.DMA],
        compiler_params=params(),
        name="ends",
    )(idx, *slots)


def tile_at(ref, plane, row, block):
    return ref[plane, pl.ds(row, ROWS), block * LANES : (block + 1) * LANES]


def neighbours(ref, plane, row, above, below, blocks, block):
    centre = tile_at(ref, plane, row, block)
    r, c = rows_of(centre.shape), lanes_of(centre.shape)
    zero = jnp.zeros_like(centre)
    right = tile_at(ref, plane, row, block + 1) if block + 1 < blocks else zero
    left = tile_at(ref, plane, row, block - 1) if block else zero
    return centre, (
        (tile_at(ref, plane + 1, row, block), tile_at(ref, plane - 1, row, block)),
        (
            pltpu.roll(jnp.where(r == 0, tile_at(ref, plane, above, block), centre), ROWS - 1, 0),
            pltpu.roll(jnp.where(r == ROWS - 1, tile_at(ref, plane, below, block), centre), 1, 0),
        ),
        (
            pltpu.roll(jnp.where(c == 0, right, centre), LANES - 1, 1),
            pltpu.roll(jnp.where(c == LANES - 1, left, centre), 1, 1),
        ),
    )


def stepped(e_ref, k_ref, u_ref, plane, tile, tiles, blocks, block):
    row = pl.multiple_of(tile * ROWS, ROWS)
    above = pl.multiple_of(jnp.minimum(row + ROWS, (tiles - 1) * ROWS), ROWS)
    below = pl.multiple_of(jnp.maximum(row - ROWS, 0), ROWS)
    e, es = neighbours(e_ref, plane + 1, row, above, below, blocks, block)
    k, ks = neighbours(k_ref, plane + 1, row, above, below, blocks, block)
    change = None
    for d in range(3):
        (e_up, e_low), (k_up, k_low) = es[d], ks[d]
        speed = u_ref[d, plane, pl.ds(row, ROWS), block * LANES : (block + 1) * LANES]
        gain = (0.5 * (k + k_up) - jnp.minimum(speed, 0.0)) * (e_up - e)
        loss = (0.5 * (k + k_low) + jnp.maximum(speed, 0.0)) * (e - e_low)
        change = gain - loss if change is None else change + (gain - loss)
    return e + change


def gather_fields(parts, rows, me, ekts, us, e, k, u, edge, sem):
    copies = []
    for slot in range(parts):
        plane = lax.rem(me - slot + parts, parts)
        ekt, main = ekts[slot], pl.ds(ROWS, rows)
        if e is not None:
            copies.append(pltpu.make_async_copy(ekt.at[pl.ds(0, rows)], e.at[plane + 1, main], sem))
        copies.append(pltpu.make_async_copy(ekt.at[pl.ds(rows, rows)], k.at[plane + 1, main], sem))
        if edge is not None:
            copies.append(
                pltpu.make_async_copy(ekt.at[pl.ds(2 * rows, EDGE)], edge.at[plane + 1], sem)
            )
        for d in range(3):
            copies.append(
                pltpu.make_async_copy(us[slot].at[pl.ds(d * rows, rows)], u.at[d, plane, main], sem)
            )
    return copies


def first_body(parts, rows, blocks, idx, *refs):
    ekts, us, (lo, hi) = refs[:parts], refs[parts : 2 * parts], refs[2 * parts : 2 * parts + 2]
    half, half_lo, half_hi, e, k, u, edge, sem = refs[2 * parts + 2 :]
    me = idx[0]
    copies = gather_fields(parts, rows, me, ekts, us, e, k, u, edge, sem)
    main = pl.ds(ROWS, rows)
    for ref, plane in ((lo, 0), (hi, parts + 1)):
        copies += [
            pltpu.make_async_copy(ref.at[pl.ds(0, rows)], e.at[plane, main], sem),
            pltpu.make_async_copy(ref.at[pl.ds(rows, rows)], k.at[plane, main], sem),
            pltpu.make_async_copy(ref.at[pl.ds(2 * rows, EDGE)], edge.at[plane], sem),
        ]
    for copy in copies:
        copy.start()
    for copy in copies:
        copy.wait()
    last = ROWS + rows
    for plane in range(parts + 2):
        top, bottom = edge[plane, :ROWS], edge[plane, ROWS:]
        e[plane, :ROWS], e[plane, last:] = down(top, 6), bottom
        k[plane, :ROWS], k[plane, last:] = down(top, 4), down(bottom, -2)
        if 0 < plane <= parts:
            for d in range(3):
                u[d, plane - 1, :ROWS] = down(top, 3 - d)
                u[d, plane - 1, last:] = down(bottom, -4 - d)
    tiles = rows // ROWS + 2

    def tile_step(n, _):
        plane, tile = n // tiles, n % tiles
        outside = ((tile == 0) & (me == 0)) | ((tile == tiles - 1) & (me == parts - 1))
        for block in range(blocks):
            value = stepped(e, k, u, plane, tile, tiles, blocks, block)
            half[plane, pl.ds(pl.multiple_of(tile * ROWS, ROWS), ROWS), block * LANES : (block + 1) * LANES] = (
                jnp.where(outside, 0.0, value)
            )
        return 0

    lax.fori_loop(0, parts * tiles, tile_step, 0)
    half_lo[...] = half[0, ROWS:last]
    half_hi[...] = half[parts - 1, ROWS:last]


def first_step(idx, ekts, us, lo, hi):
    parts, width = len(ekts), lo.shape[1]
    rows = (lo.shape[0] - EDGE) // 2
    tall = rows + 2 * ROWS
    plane = jax.ShapeDtypeStruct((rows, width), F32)
    return pl.pallas_call(
        functools.partial(first_body, parts, rows, width // LANES),
        out_shape=[jax.ShapeDtypeStruct((parts, tall, width), F32), plane, plane],
        in_specs=[SMEM] + [ANY] * (2 * parts + 2),
        out_specs=[VMEM] * 3,
        scratch_shapes=[
            pltpu.VMEM((parts + 2, tall, width), F32),
            pltpu.VMEM((parts + 2, tall, width), F32),
            pltpu.VMEM((3, parts, tall, width), F32),
            pltpu.VMEM((parts + 2, EDGE, width), F32),
            pltpu.SemaphoreType.DMA,
        ],
        compiler_params=params(),
        name="first_step",
    )(idx, *ekts, *us, lo, hi)


def second_body(parts, rows, blocks, idx, *refs):
    ekts, us = refs[:parts], refs[parts : 2 * parts]
    lo, hi, half, half_lo, half_hi = refs[2 * parts : 2 * parts + 5]
    refs = refs[2 * parts + 5 :]
    pieces, (sums, e, k, u, edge, result, sem) = refs[:blocks], refs[blocks:]
    me, my = idx[0], idx[1]
    copies = gather_fields(parts, rows, me, ekts, us, None, k, u, edge, sem)
    main = pl.ds(ROWS, rows)
    for ref, plane in ((lo, 0), (hi, parts + 1)):
        copies.append(pltpu.make_async_copy(ref.at[pl.ds(rows, rows)], k.at[plane, main], sem))
    copies.append(pltpu.make_async_copy(half, e.at[pl.ds(1, parts)], sem))
    copies.append(pltpu.make_async_copy(half_lo, e.at[0, main], sem))
    copies.append(pltpu.make_async_copy(half_hi, e.at[parts + 1, main], sem))
    for copy in copies:
        copy.start()
    for copy in copies:
        copy.wait()
    last = ROWS + rows
    for plane in range(1, parts + 1):
        top, bottom = edge[plane, :ROWS], edge[plane, ROWS:]
        k[plane, :ROWS], k[plane, last:] = down(top, 4), down(bottom, -2)
    tiles = rows // ROWS + 2
    shape = (ROWS, LANES)
    row, lane = rows_of(shape), lanes_of(shape)

    def plane_step(plane, found):
        def tile_step(tile, total):
            at = pl.multiple_of((tile - 1) * ROWS, ROWS)
            for block in range(blocks):
                value = stepped(e, k, u, plane, tile, tiles, blocks, block)
                result[plane, pl.ds(at, ROWS), block * LANES : (block + 1) * LANES] = value
                total = total + value
            return total

        total = lax.fori_loop(1, tiles - 1, tile_step, jnp.zeros(shape, F32))
        return jnp.where((lane == plane), jnp.sum(total), found)

    sums[...] = lax.fori_loop(0, parts, plane_step, jnp.zeros(shape, F32))
    out = []
    for n, piece in enumerate(pieces):
        block = pl.multiple_of(jnp.bitwise_xor(my, n) * LANES, LANES)
        copy = pltpu.make_async_copy(result.at[:, :, pl.ds(block, LANES)], piece, sem)
        copy.start()
        out.append(copy)
    for copy in out:
        copy.wait()


def second_step(idx, ekts, us, lo, hi, half, half_lo, half_hi):
    parts, (rows, width) = len(ekts), half_lo.shape
    tall, blocks = rows + 2 * ROWS, width // LANES
    out = pl.pallas_call(
        functools.partial(second_body, parts, rows, blocks),
        out_shape=[jax.ShapeDtypeStruct((parts, rows, LANES), F32)] * blocks
        + [jax.ShapeDtypeStruct((ROWS, LANES), F32)],
        in_specs=[SMEM] + [ANY] * (2 * parts + 5),
        out_specs=[ANY] * blocks + [VMEM],
        scratch_shapes=[
            pltpu.VMEM((parts + 2, tall, width), F32),
            pltpu.VMEM((parts + 2, tall, width), F32),
            pltpu.VMEM((3, parts, tall, width), F32),
            pltpu.VMEM((parts + 2, EDGE, width), F32),
            pltpu.VMEM((parts, rows, width), F32),
            pltpu.SemaphoreType.DMA,
        ],
        compiler_params=params(),
        name="second_step",
    )(idx, *ekts, *us, lo, hi, half, half_lo, half_hi)
    return out[:blocks], out[blocks]


def place_body(count, parts, idx, *refs):
    pieces, out, sem = refs[:count], *refs[count:]
    copies = []
    for n, piece in enumerate(pieces):
        at = jnp.bitwise_xor(idx[1], n) * parts
        copies.append(pltpu.make_async_copy(piece, out.at[pl.ds(at, parts)], sem))
        copies[-1].start()
    for copy in copies:
        copy.wait()


def place(idx, pieces):
    parts, rows, lanes = pieces[0].shape
    return pl.pallas_call(
        functools.partial(place_body, len(pieces), parts),
        out_shape=jax.ShapeDtypeStruct((parts * len(pieces), rows, lanes), F32),
        in_specs=[SMEM] + [ANY] * len(pieces),
        out_specs=ANY,
        scratch_shapes=[pltpu.SemaphoreType.DMA],
        compiler_params=params(),
        name="place",
    )(idx, *pieces)


def means_body(parts, planes, cells, idx, found, mean, running):
    first = idx[2] * (planes // parts)
    values = found[...]
    shape = (planes, values.shape[0])
    group = lax.broadcasted_iota(jnp.int32, shape, 1) // parts
    mine = first + lax.broadcasted_iota(jnp.int32, shape, 0) // parts
    own = (group == mine).astype(F32)
    lower = (group < mine).astype(F32)
    dot = functools.partial(jnp.dot, precision=lax.Precision.HIGHEST, preferred_element_type=F32)
    own, lower = dot(own, values), dot(lower, values)
    lane, plane = lanes_of(own.shape), rows_of(own.shape)
    within = plane % parts
    total = jnp.sum(jnp.where(lane == within, own, 0.0), 1, keepdims=True)
    until = jnp.sum(
        jnp.where(lane < parts, lower, 0.0) + jnp.where(lane <= within, own, 0.0), 1, keepdims=True
    )
    rank = (first * parts + plane[:, :1] + 1).astype(F32)
    mean[...] = total / cells
    running[...] = until / cells / rank


def means(idx, found, parts, planes, cells):
    shape = jax.ShapeDtypeStruct((planes, 1), F32)
    return pl.pallas_call(
        functools.partial(means_body, parts, planes, cells),
        out_shape=[shape] * 2,
        in_specs=[SMEM, VMEM],
        out_specs=[VMEM] * 2,
        compiler_params=params(),
        name="means",
    )(idx, found)


def shift(size, by):
    return [(i, (i + by) % size) for i in range(size)]


def per_device(energy, flow):
    parts, sides, stacks = (lax.axis_size(a) for a in ("gx", "gy", "gz"))
    idx = jnp.stack([lax.axis_index(a) for a in ("gx", "gy", "gz")]).astype(jnp.int32)
    sent = pack(idx, energy, flow, parts, tuple(range(1, parts)))
    ekts = [lax.ppermute(ekt, "gx", shift(parts, n + 1)) for n, (ekt, _) in enumerate(sent)]
    us = [lax.ppermute(u, "gx", shift(parts, n + 1)) for n, (_, u) in enumerate(sent)]
    own = pack(idx, energy, flow, parts, (0,))[0]
    ekts, us = [own[0]] + ekts, [own[1]] + us

    line = ("gy", "gz")
    around = [(n % sides) * stacks + n // sides for n in range(stacks * sides)]
    up = list(zip(around, around[1:] + around[:1]))
    down_ = [(b, a) for a, b in up]
    lowest, highest = ends(idx, ekts)
    lo, hi = lax.ppermute(highest, line, up), lax.ppermute(lowest, line, down_)
    half, half_low, half_high = first_step(idx, ekts, us, lo, hi)
    half_lo, half_hi = lax.ppermute(half_high, line, up), lax.ppermute(half_low, line, down_)
    pieces, sums = second_step(idx, ekts, us, lo, hi, half, half_lo, half_hi)

    pieces = [pieces[0]] + [
        lax.ppermute(piece, "gy", [(i, i ^ (n + 1)) for i in range(sides)])
        for n, piece in enumerate(pieces[1:])
    ]
    energy_next = place(idx, pieces)

    everyone = ("gz", "gy", "gx")
    count = parts * sides * stacks
    copies = jnp.broadcast_to(sums[:1, :ROWS], (count, ROWS))
    found = lax.all_to_all(copies, everyone, 0, 0, tiled=True)
    cells = energy.shape[1] * energy.shape[2]
    mean, running = means(idx, found, parts, parts * sides, cells)
    return energy_next, mean[:, 0], running[:, 0]


def solution(mesh):
    placed = (P(("gz", "gy", "gx"), None, None), P(None, ("gz", "gy", "gx"), None, None))
    return jax.shard_map(
        per_device,
        mesh=mesh,
        in_specs=placed,
        out_specs=(P("gz", "gx", "gy"), P("gz"), P("gz")),
        check_vma=False,
    )
```

```python
import functools

import jax
import jax.numpy as jnp
from jax import lax
from jax.experimental import pallas as pl
from jax.experimental.pallas import tpu as pltpu
from jax.sharding import PartitionSpec as P

F32 = jnp.float32
ANY = pl.BlockSpec(memory_space=pl.ANY)
SMEM = pl.BlockSpec(memory_space=pltpu.SMEM)
VMEM = pl.BlockSpec(memory_space=pltpu.VMEM)
HBM = pl.BlockSpec(memory_space=pltpu.HBM)
LANES = 128
ROWS = 8
FIRST = 32
UNROLL = 4


def params(mib=24):
    return pltpu.CompilerParams(vmem_limit_bytes=mib * 2**20)


def rows_of(shape):
    return lax.broadcasted_iota(jnp.int32, shape, 0)


def lanes_of(shape):
    return lax.broadcasted_iota(jnp.int32, shape, 1)


def down(tile, count):
    count %= ROWS
    return pltpu.roll(tile, count, 0) if count else tile


def part_rows(rows, cut):
    rest = rows - cut
    return (5 * cut + ROWS, 2 * rest + ROWS, 3 * rest)


def edge_row(part, rows, cut):
    return 2 * (rows - cut if part else cut)


def segments(field, rows, cut, begin, end):
    rest, found = rows - cut, []
    low, high = max(begin, 0), min(end, cut)
    if low < high:
        at = field * cut if field < 2 else field * cut + ROWS
        found.append((0, at + low, low, high - low))
    low, high = max(begin, cut), min(end, rows)
    if low < high:
        part, at = (1, field * rest) if field < 2 else (2, (field - 2) * rest)
        found.append((part, at + low - cut, low, high - low))
    return found


def pack_body(quarters, rows, cut, slots, parts, idx, energy, flow, *refs):
    count = len(slots) * len(parts)
    outs, (low, high, sem, tile_sem) = refs[:count], refs[count:]
    me = idx[0]
    fields = [energy.at[0]] + [flow.at[c, 0] for c in (3, 0, 1, 2)]
    copies, tiles = [], []
    for n, slot in enumerate(slots):
        first = pl.multiple_of(lax.rem(me + slot, quarters) * rows, ROWS)
        before = pl.multiple_of(jnp.maximum(first - ROWS, 0), ROWS)
        after = pl.multiple_of(jnp.minimum(first + rows, (quarters - 1) * rows), ROWS)
        for f, field in enumerate(fields):
            if 0 in parts:
                tiles.append(
                    pltpu.make_async_copy(field.at[pl.ds(before, ROWS)], low.at[n, f], tile_sem)
                )
            if 1 in parts:
                tiles.append(
                    pltpu.make_async_copy(field.at[pl.ds(after, ROWS)], high.at[n, f], tile_sem)
                )
    for copy in tiles:
        copy.start()
    for n, slot in enumerate(slots):
        first = lax.rem(me + slot, quarters) * rows
        for f, field in enumerate(fields):
            for part, at, row, size in segments(f, rows, cut, 0, rows):
                if part in parts:
                    out = outs[n * len(parts) + parts.index(part)]
                    source = field.at[pl.ds(pl.multiple_of(first + row, ROWS), size)]
                    copies.append(pltpu.make_async_copy(source, out.at[pl.ds(at, size)], sem))
    for copy in copies:
        copy.start()
    for copy in tiles:
        copy.wait()
    shape = low.shape[2:]
    row = rows_of(shape)
    places = ((0, 2), (2, 2), (4, 1), (5, 1), (6, 1))
    for n, slot in enumerate(slots):
        to = lax.rem(me + slot, quarters)
        for part in parts:
            if part == 2:
                continue
            tile = jnp.zeros(shape, F32)
            for f, (begin, size) in enumerate(places):
                here = (row >= begin) & (row < begin + size)
                moved = down(high[n, f], begin) if part else down(low[n, f], begin + size)
                tile = jnp.where(here, moved, tile)
            out = outs[n * len(parts) + parts.index(part)]
            at = edge_row(part, rows, cut)
            out[at : at + ROWS] = jnp.where(to == (quarters - 1 if part else 0), 0.0, tile)
    for copy in copies:
        copy.wait()


def pack(idx, energy, flow, quarters, cut, slots, parts):
    rows, width = energy.shape[1] // quarters, energy.shape[2]
    sizes = part_rows(rows, cut)
    shapes = [jax.ShapeDtypeStruct((sizes[part], width), F32) for part in parts] * len(slots)
    out = pl.pallas_call(
        functools.partial(pack_body, quarters, rows, cut, slots, parts),
        out_shape=shapes,
        in_specs=[SMEM, HBM, HBM],
        out_specs=[VMEM] * len(shapes),
        scratch_shapes=[
            pltpu.VMEM((len(slots), 5, ROWS, width), F32),
            pltpu.VMEM((len(slots), 5, ROWS, width), F32),
            pltpu.SemaphoreType.DMA,
            pltpu.SemaphoreType.DMA,
        ],
        compiler_params=params(),
        name="pack",
    )(idx, energy, flow)
    return [list(out[n * len(parts) : (n + 1) * len(parts)]) for n in range(len(slots))]


def end_planes(idx, quarters):
    above = lax.rem(idx[1], 2) == 0
    return jnp.where(above, quarters - 1, 0), jnp.where(above, 0, quarters - 1)


def beyond(plane):
    return jnp.where(plane == 0, 0, plane + 2)


def ends_body(count, idx, *refs):
    slots, outs = refs[:count], refs[count:]
    for slot, ref in enumerate(slots):
        plane = lax.rem(idx[0] - slot + count, count)
        for wanted, out in zip(end_planes(idx, count), outs):

            @pl.when(plane == wanted)
            def _():
                out[...] = ref[: out.shape[0]]


def ends(idx, slots, rows):
    shape = jax.ShapeDtypeStruct((rows, slots[0].shape[1]), F32)
    return pl.pallas_call(
        functools.partial(ends_body, len(slots)),
        out_shape=[shape] * 2,
        in_specs=[SMEM] + [VMEM] * len(slots),
        out_specs=[VMEM] * 2,
        compiler_params=params(),
        name="ends",
    )(idx, *slots)


def tile_at(ref, plane, row, block):
    return ref[plane, pl.ds(row, ROWS), block * LANES : (block + 1) * LANES]


def neighbours(ref, plane, row, above, below, blocks, block):
    centre = tile_at(ref, plane, row, block)
    r, c = rows_of(centre.shape), lanes_of(centre.shape)
    zero = jnp.zeros_like(centre)
    right = tile_at(ref, plane, row, block + 1) if block + 1 < blocks else zero
    left = tile_at(ref, plane, row, block - 1) if block else zero
    return centre, (
        (tile_at(ref, plane + 1, row, block), tile_at(ref, plane - 1, row, block)),
        (
            pltpu.roll(jnp.where(r == 0, tile_at(ref, plane, above, block), centre), ROWS - 1, 0),
            pltpu.roll(jnp.where(r == ROWS - 1, tile_at(ref, plane, below, block), centre), 1, 0),
        ),
        (
            pltpu.roll(jnp.where(c == 0, right, centre), LANES - 1, 1),
            pltpu.roll(jnp.where(c == LANES - 1, left, centre), 1, 1),
        ),
    )


def stepped(e_ref, k_ref, u_ref, plane, row, blocks, block):
    row = pl.multiple_of(row, ROWS)
    above = pl.multiple_of(jnp.minimum(row + ROWS, e_ref.shape[1] - ROWS), ROWS)
    below = pl.multiple_of(jnp.maximum(row - ROWS, 0), ROWS)
    e, es = neighbours(e_ref, plane + 1, row, above, below, blocks, block)
    k, ks = neighbours(k_ref, plane + 1, row, above, below, blocks, block)
    change = None
    for d in range(3):
        (e_up, e_low), (k_up, k_low) = es[d], ks[d]
        speed = u_ref[d, plane, pl.ds(row, ROWS), block * LANES : (block + 1) * LANES]
        gain = (0.5 * (k + k_up) - jnp.minimum(speed, 0.0)) * (e_up - e)
        loss = (0.5 * (k + k_low) + jnp.maximum(speed, 0.0)) * (e - e_low)
        change = gain - loss if change is None else change + (gain - loss)
    return e + change


def gather_rows(rows, cut, window, span, me, slots, ends, e, k, u):
    begin, end = window
    quarters = len(slots)
    planes = [(lax.rem(me - s + quarters, quarters), parts, True) for s, parts in enumerate(slots)]
    for plane, parts, inside in planes + [(*pair, False) for pair in ends]:
        up = plane + 1 if inside else plane
        for field in range(5 if inside else 2):
            if field == 0 and e is None:
                continue
            for part, at, row, size in segments(
                field, rows, cut, *(window if field < 2 else span)
            ):
                to, value = pl.ds(row - begin, size), parts[part][at : at + size]
                if field < 2:
                    (e, k)[field][up, to] = value
                else:
                    u[field - 2, plane, to] = value
        if begin < 0:
            tile = parts[0][2 * cut : 2 * cut + ROWS]
            if e is not None:
                e[up, :ROWS] = down(tile, 6)
            k[up, :ROWS] = down(tile, 4)
            for d in range(3 if inside and span[0] < 0 else 0):
                u[d, plane, :ROWS] = down(tile, 3 - d)
        if end > rows:
            tile = parts[1][2 * (rows - cut) : 2 * (rows - cut) + ROWS]
            to = pl.ds(end - begin - ROWS, ROWS)
            if e is not None:
                e[up, to] = tile
            k[up, to] = down(tile, -2)
            for d in range(3 if inside and span[1] > rows else 0):
                u[d, plane, to] = down(tile, -4 - d)


def scratch(quarters, tall, width):
    return [
        pltpu.VMEM((quarters + 2, tall, width), F32),
        pltpu.VMEM((quarters + 2, tall, width), F32),
        pltpu.VMEM((3, quarters, tall, width), F32),
    ]


def grouped(refs, counts):
    out = []
    for count in counts:
        out.append(refs[:count])
        refs = refs[count:]
    return out + [refs]


def first_body(rows, cut, window, span, sent, quarters, blocks, given, idx, *refs):
    *slots, even, odd, refs = grouped(refs, [given[0]] * quarters + [given[1]] * 2)
    half, *half_ends, e, k, u = refs
    me = idx[0]
    last = end_planes(idx, quarters)
    ends = [(beyond(plane), parts) for plane, parts in zip(last, (even, odd))]
    gather_rows(rows, cut, window, span, me, slots, ends, e, k, u)
    begin = window[0]
    tiles = (span[1] - span[0]) // ROWS

    def tile_step(n, _):
        plane, at = n // tiles, span[0] + (n % tiles) * ROWS
        outside = ((at < 0) & (me == 0)) | ((at >= rows) & (me == quarters - 1))
        to = pl.ds(pl.multiple_of(at - span[0], ROWS), ROWS)
        for block in range(blocks):
            value = stepped(e, k, u, plane, at - begin, blocks, block)
            value = jnp.where(outside, 0.0, value)
            half[plane, to, block * LANES : (block + 1) * LANES] = value
        return 0

    lax.fori_loop(0, quarters * tiles, tile_step, 0, unroll=UNROLL)
    for plane, ref in zip(last, half_ends):
        ref[...] = half[plane, sent[0] - span[0] : sent[1] - span[0]]


def first_step(idx, slots, even, odd, rows, cut, window, span, sent):
    quarters, width = len(slots), even[0].shape[1]
    given = (len(slots[0]), len(even))
    flat = [x for parts in slots for x in parts] + list(even) + list(odd)
    plane = jax.ShapeDtypeStruct((sent[1] - sent[0], width), F32)
    return pl.pallas_call(
        functools.partial(
            first_body, rows, cut, window, span, sent, quarters, width // LANES, given
        ),
        out_shape=[jax.ShapeDtypeStruct((quarters, span[1] - span[0], width), F32), plane, plane],
        in_specs=[SMEM] + [VMEM] * len(flat),
        out_specs=[VMEM] * 3,
        scratch_shapes=scratch(quarters, window[1] - window[0], width),
        compiler_params=params(),
        name="first_step",
    )(idx, *flat)


def second_body(rows, cut, window, span, quarters, blocks, given, halves, before, idx, *refs):
    *slots, even, odd, half, half_even, half_odd, early, pieces, refs = grouped(
        refs, [given[0]] * quarters + [given[1]] * 2 + [len(halves)] * 3 + [before, blocks // 2]
    )
    total_ref, e, k, u, result, totals = refs
    me, my = idx[0], idx[1]
    outer = [beyond(plane) for plane in end_planes(idx, quarters)]
    ends = list(zip(outer, (even, odd)))
    gather_rows(rows, cut, window, span, me, slots, ends, None, k, u)
    begin = window[0]
    for ref, *sides, (start, row, end) in zip(half, half_even, half_odd, halves):
        if start < end:
            for plane in range(quarters):
                e[plane + 1, row - begin : end - begin] = ref[plane, row - start : end - start]
        first, last = max(row, span[0]), min(end, span[1])
        if first >= last:
            continue
        at = max(start, 0)
        for plane, side in zip(outer, sides):
            e[plane, first - begin : last - begin] = side[first - at : last - at]
    tiles = (span[1] - span[0]) // ROWS
    totals[...] = jnp.zeros(totals.shape, F32)

    def tile_step(n, _):
        plane, at = n // tiles, pl.multiple_of((n % tiles) * ROWS, ROWS)
        values = []
        for block in range(blocks):
            value = stepped(e, k, u, plane, at + (span[0] - begin), blocks, block)
            result[plane, pl.ds(at, ROWS), block * LANES : (block + 1) * LANES] = value
            values.append(value)
        while len(values) > 1:
            values = [a + b for a, b in zip(values[0::2], values[1::2])]
        totals[plane] = totals[plane] + values[0]
        return 0

    lax.fori_loop(0, quarters * tiles, tile_step, 0, unroll=UNROLL)
    lane = lanes_of((ROWS, LANES))
    found = jnp.zeros((ROWS, LANES), F32)
    for plane in range(quarters):
        found = jnp.where(lane == my * quarters + plane, jnp.sum(totals[plane]), found)
    for n in range(blocks):
        lanes = pl.ds(pl.multiple_of(jnp.bitwise_xor(my, n) * LANES, LANES), LANES)
        pieces[n // 2][n % 2] = result[:, :, lanes]
    if before:
        total_ref[...] = jnp.broadcast_to((early[0][...] + found)[:1], total_ref.shape)
    else:
        total_ref[...] = found


def second_step(
    idx, slots, even, odd, half, half_even, half_odd, early, rows, cut, window, span, halves, count
):
    quarters, width = len(slots), half[0].shape[2]
    given, blocks, size = (len(slots[0]), len(even)), width // LANES, span[1] - span[0]
    flat = [x for parts in slots for x in parts] + list(even) + list(odd)
    flat += list(half) + list(half_even) + list(half_odd) + list(early)
    before = len(early)
    shapes = [jax.ShapeDtypeStruct((2, quarters, size, LANES), F32)] * (blocks // 2)
    shapes += [jax.ShapeDtypeStruct((count if before else ROWS, LANES), F32)]
    out = pl.pallas_call(
        functools.partial(
            second_body, rows, cut, window, span, quarters, blocks, given, halves, before
        ),
        out_shape=shapes,
        in_specs=[SMEM] + [VMEM] * len(flat),
        out_specs=[VMEM] * len(shapes),
        scratch_shapes=scratch(quarters, window[1] - window[0], width)
        + [pltpu.VMEM((quarters, size, width), F32), pltpu.VMEM((quarters, ROWS, LANES), F32)],
        compiler_params=params(),
        name="second_step",
    )(idx, *flat)
    return out[:-1], out[-1]


def pass_on_body(counts, *refs):
    *groups, (out,) = grouped(refs, counts)
    row = 0
    for group in groups:
        size = group[0].shape[2]
        for n, pair in enumerate(group):
            out[n, :, row : row + size] = pair[1]
        row += size


def pass_on(groups):
    _, quarters, _, lanes = groups[0][0].shape
    rows = sum(group[0].shape[2] for group in groups)
    flat = [pair for group in groups for pair in group]
    return pl.pallas_call(
        functools.partial(pass_on_body, [len(group) for group in groups]),
        out_shape=jax.ShapeDtypeStruct((len(groups[0]), quarters, rows, lanes), F32),
        in_specs=[VMEM] * len(flat),
        out_specs=VMEM,
        compiler_params=params(),
        name="pass_on",
    )(*flat)


def finish_body(counts, quarters, cells, idx, found, passed, *refs):
    *groups, (out, mean, running, held, sem, held_sem) = grouped(refs, counts)
    my, pieces, row = idx[1], [], 0

    def planes_from(n):
        return pl.ds(jnp.bitwise_xor(my, n) * quarters, quarters)

    for n in range(counts[0]):
        to = out.at[planes_from(2 * n + 1)]
        pieces.append(pltpu.make_async_copy(passed.at[n], to, sem))
    for group in groups:
        size = group[0].shape[2]
        for n, pair in enumerate(group):
            to = out.at[planes_from(2 * n), pl.ds(row, size)]
            pieces.append(pltpu.make_async_copy(pair.at[0], to, sem))
        row += size
    for copy in pieces:
        copy.start()
    planes, stack = held.shape[2], idx[2]

    def stack_sum(stack):
        rows = found[pl.ds(pl.multiple_of(stack * planes, ROWS), planes)]
        tiles = [rows[n : n + ROWS] for n in range(0, planes, ROWS)]
        while len(tiles) > 1:
            tiles = [a + b for a, b in zip(tiles[0::2], tiles[1::2])]
        return tiles[0]

    here = jnp.sum(stack_sum(stack), 0, keepdims=True)
    zero = jnp.zeros((ROWS, LANES), F32)
    lower = lax.fori_loop(0, stack, lambda n, total: total + stack_sum(n), zero)
    lane = lanes_of(here.shape)
    here = here / cells
    until, by = here, 1
    while by < planes:
        until = until + jnp.where(lane >= by, pltpu.roll(until, by, 1), 0.0)
        by *= 2
    until = until + jnp.sum(lower) / cells
    rank = (stack * planes + lane + 1).astype(F32)
    held[0] = here[:, :planes]
    held[1] = (until / rank)[:, :planes]
    lines = [
        pltpu.make_async_copy(held.at[n], line, held_sem) for n, line in enumerate((mean, running))
    ]
    for copy in lines:
        copy.start()
    for copy in pieces + lines:
        copy.wait()


def finish(idx, found, passed, groups, cells):
    pairs, quarters, rows, lanes = passed.shape
    flat = [pair for group in groups for pair in group]
    counts = [len(group) for group in groups]
    planes = 2 * pairs * quarters
    line = jax.ShapeDtypeStruct((1, planes), F32)
    return pl.pallas_call(
        functools.partial(finish_body, counts, quarters, cells),
        out_shape=[jax.ShapeDtypeStruct((planes, rows, lanes), F32), line, line],
        in_specs=[SMEM, VMEM] + [ANY] * (1 + len(flat)),
        out_specs=[ANY] * 3,
        scratch_shapes=[
            pltpu.VMEM((2, 1, planes), F32),
            pltpu.SemaphoreType.DMA,
            pltpu.SemaphoreType.DMA,
        ],
        compiler_params=params(),
        name="finish",
    )(idx, found, passed, *flat)


def shift(size, by):
    return [(i, (i + by) % size) for i in range(size)]


def over_chips(pairs, sides):
    got = [pairs[0]]
    for n, pair in enumerate(pairs[1:], 1):
        where = [(i, i ^ (2 * n)) for i in range(sides)]
        got.append(lax.ppermute(pair, "gy", where))
    return got


def both_steps(energy, flow):
    quarters, sides, stacks = (lax.axis_size(a) for a in ("gx", "gy", "gz"))
    idx = jnp.stack([lax.axis_index(a) for a in ("gx", "gy", "gz")]).astype(jnp.int32)
    rows, cut = energy.shape[1] // quarters, FIRST
    done = cut - ROWS
    cells = energy.shape[1] * energy.shape[2]
    energy = pltpu.with_memory_space_constraint(energy, pltpu.HBM)
    flow = pltpu.with_memory_space_constraint(flow, pltpu.HBM)

    others = (1, *range(quarters - 1, 1, -1))
    sent = pack(idx, energy, flow, quarters, cut, others, (0,))
    later = pack(idx, energy, flow, quarters, cut, others, (1, 2))
    sent = {slot: a + b for slot, a, b in zip(others, sent, later)}
    got = {
        (slot, part): lax.ppermute(sent[slot][part], "gx", shift(quarters, slot))
        for part in range(3)
        for slot in others
    }
    own = pack(idx, energy, flow, quarters, cut, (0,), (0, 1, 2))[0]
    slots = [own] + [[got[slot, part] for part in range(3)] for slot in range(1, quarters)]
    firsts = [parts[:1] for parts in slots]

    def place_of(stack):
        stack %= stacks * sides
        return (stack % sides) * stacks + stack // sides

    def exchanged(even, odd):
        got = []
        for start, value in ((1, odd), (0, even)):
            lows = [(place_of(n), place_of(n + 1)) for n in range(start, stacks * sides, 2)]
            pairs = lows + [(b, a) for a, b in lows]
            got.append(lax.ppermute(value, ("gy", "gz"), pairs))
        return got[1], got[0]

    last = ends(idx, [s[0] for s in slots], 2 * cut + ROWS)
    even, odd = ([x] for x in exchanged(*last))
    args = (rows, cut, (-ROWS, cut), (-ROWS, cut), (0, done))
    half_a, *last = first_step(idx, firsts, even, odd, *args)
    even_a, odd_a = exchanged(*last)
    args = ([half_a], [even_a], [odd_a], (), rows, cut, (-ROWS, cut), (0, done))
    args += (((-ROWS, -ROWS, cut),), 0)
    pieces_a, sums = second_step(idx, firsts, even, odd, *args)
    pieces_a = over_chips(pieces_a, sides)

    last = ends(idx, [s[1] for s in slots], 2 * (rows - cut) + ROWS)
    even, odd = (a + [b] for a, b in zip((even, odd), exchanged(*last)))
    top = rows + ROWS
    args = (rows, cut, (done - ROWS, top), (done, top), (done, rows))
    half_b, *last = first_step(idx, slots, even, odd, *args)
    even_b, odd_b = exchanged(*last)
    args = ([half_a, half_b], [even_a, even_b], [odd_a, odd_b], (sums,), rows, cut)
    args += ((done - ROWS, top), (done, rows), ((-ROWS, done - ROWS, done), (done, done, top)))
    args += (quarters * sides * stacks,)
    pieces_b, sums = second_step(idx, slots, even, odd, *args)
    pieces_b = over_chips(pieces_b, sides)

    everyone = functools.partial(lax.all_to_all, tiled=True)
    found = everyone(sums, ("gz", "gy", "gx"), 0, 0)
    groups = [pieces_a, pieces_b]
    passed = pass_on(groups)
    passed = lax.ppermute(passed, "gy", [(i, i ^ 1) for i in range(sides)])
    out = finish(idx, found, passed, groups, cells)
    return out[0], out[1].reshape(-1), out[2].reshape(-1)


def solution(mesh):
    placed = (P(("gz", "gy", "gx"), None, None), P(None, ("gz", "gy", "gx"), None, None))
    return jax.shard_map(
        both_steps,
        mesh=mesh,
        in_specs=placed,
        out_specs=(P("gz", "gx", "gy"), P("gz"), P("gz")),
        check_vma=False,
    )
```

```python
import functools

import jax
import jax.numpy as jnp
from jax import lax
from jax.experimental import pallas as pl
from jax.experimental.pallas import tpu as pltpu
from jax.sharding import PartitionSpec as P

F32 = jnp.float32
ANY = pl.BlockSpec(memory_space=pl.ANY)
SMEM = pl.BlockSpec(memory_space=pltpu.SMEM)
VMEM = pl.BlockSpec(memory_space=pltpu.VMEM)
HBM = pl.BlockSpec(memory_space=pltpu.HBM)
LANES = 128
ROWS = 8
FIRST = 32
UNROLL = 4


def params(mib=24):
    return pltpu.CompilerParams(vmem_limit_bytes=mib * 2**20)


def rows_of(shape):
    return lax.broadcasted_iota(jnp.int32, shape, 0)


def lanes_of(shape):
    return lax.broadcasted_iota(jnp.int32, shape, 1)


def down(tile, count):
    count %= ROWS
    return pltpu.roll(tile, count, 0) if count else tile


def part_rows(rows, cut):
    rest = rows - cut
    return (5 * cut + ROWS, 2 * rest + ROWS, 3 * rest)


def edge_row(part, rows, cut):
    return 2 * (rows - cut if part else cut)


def segments(field, rows, cut, begin, end):
    rest, found = rows - cut, []
    low, high = max(begin, 0), min(end, cut)
    if low < high:
        at = field * cut if field < 2 else field * cut + ROWS
        found.append((0, at + low, low, high - low))
    low, high = max(begin, cut), min(end, rows)
    if low < high:
        part, at = (1, field * rest) if field < 2 else (2, (field - 2) * rest)
        found.append((part, at + low - cut, low, high - low))
    return found


def pack_body(quarters, rows, cut, slots, parts, idx, energy, flow, *refs):
    count = len(slots) * len(parts)
    outs, (low, high, sem, tile_sem) = refs[:count], refs[count:]
    me = idx[0]
    fields = [energy.at[0]] + [flow.at[c, 0] for c in (3, 0, 1, 2)]
    copies, tiles = [], []
    for n, slot in enumerate(slots):
        first = pl.multiple_of(lax.rem(me + slot, quarters) * rows, ROWS)
        before = pl.multiple_of(jnp.maximum(first - ROWS, 0), ROWS)
        after = pl.multiple_of(jnp.minimum(first + rows, (quarters - 1) * rows), ROWS)
        for f, field in enumerate(fields):
            if 0 in parts:
                tiles.append(
                    pltpu.make_async_copy(field.at[pl.ds(before, ROWS)], low.at[n, f], tile_sem)
                )
            if 1 in parts:
                tiles.append(
                    pltpu.make_async_copy(field.at[pl.ds(after, ROWS)], high.at[n, f], tile_sem)
                )
    for copy in tiles:
        copy.start()
    for n, slot in enumerate(slots):
        first = lax.rem(me + slot, quarters) * rows
        for f, field in enumerate(fields):
            for part, at, row, size in segments(f, rows, cut, 0, rows):
                if part in parts:
                    out = outs[n * len(parts) + parts.index(part)]
                    source = field.at[pl.ds(pl.multiple_of(first + row, ROWS), size)]
                    copies.append(pltpu.make_async_copy(source, out.at[pl.ds(at, size)], sem))
    for copy in copies:
        copy.start()
    for copy in tiles:
        copy.wait()
    shape = low.shape[2:]
    row = rows_of(shape)
    places = ((0, 2), (2, 2), (4, 1), (5, 1), (6, 1))
    for n, slot in enumerate(slots):
        to = lax.rem(me + slot, quarters)
        for part in parts:
            if part == 2:
                continue
            tile = jnp.zeros(shape, F32)
            for f, (begin, size) in enumerate(places):
                here = (row >= begin) & (row < begin + size)
                moved = down(high[n, f], begin) if part else down(low[n, f], begin + size)
                tile = jnp.where(here, moved, tile)
            out = outs[n * len(parts) + parts.index(part)]
            at = edge_row(part, rows, cut)
            out[at : at + ROWS] = jnp.where(to == (quarters - 1 if part else 0), 0.0, tile)
    for copy in copies:
        copy.wait()


def pack(idx, energy, flow, quarters, cut, slots, parts):
    rows, width = energy.shape[1] // quarters, energy.shape[2]
    sizes = part_rows(rows, cut)
    shapes = [jax.ShapeDtypeStruct((sizes[part], width), F32) for part in parts] * len(slots)
    out = pl.pallas_call(
        functools.partial(pack_body, quarters, rows, cut, slots, parts),
        out_shape=shapes,
        in_specs=[SMEM, HBM, HBM],
        out_specs=[VMEM] * len(shapes),
        scratch_shapes=[
            pltpu.VMEM((len(slots), 5, ROWS, width), F32),
            pltpu.VMEM((len(slots), 5, ROWS, width), F32),
            pltpu.SemaphoreType.DMA,
            pltpu.SemaphoreType.DMA,
        ],
        compiler_params=params(),
        name="pack",
    )(idx, energy, flow)
    return [list(out[n * len(parts) : (n + 1) * len(parts)]) for n in range(len(slots))]


def end_planes(idx, quarters):
    above = lax.rem(idx[1], 2) == 0
    return jnp.where(above, quarters - 1, 0), jnp.where(above, 0, quarters - 1)


def beyond(plane):
    return jnp.where(plane == 0, 0, plane + 2)


def ends_body(count, idx, *refs):
    slots, outs = refs[:count], refs[count:]
    for slot, ref in enumerate(slots):
        plane = lax.rem(idx[0] - slot + count, count)
        for wanted, out in zip(end_planes(idx, count), outs):

            @pl.when(plane == wanted)
            def _():
                out[...] = ref[: out.shape[0]]


def ends(idx, slots, rows):
    shape = jax.ShapeDtypeStruct((rows, slots[0].shape[1]), F32)
    return pl.pallas_call(
        functools.partial(ends_body, len(slots)),
        out_shape=[shape] * 2,
        in_specs=[SMEM] + [VMEM] * len(slots),
        out_specs=[VMEM] * 2,
        compiler_params=params(),
        name="ends",
    )(idx, *slots)


def tile_at(ref, plane, row, block):
    return ref[plane, pl.ds(row, ROWS), block * LANES : (block + 1) * LANES]


def neighbours(ref, plane, row, above, below, blocks, block):
    centre = tile_at(ref, plane, row, block)
    r, c = rows_of(centre.shape), lanes_of(centre.shape)
    zero = jnp.zeros_like(centre)
    right = tile_at(ref, plane, row, block + 1) if block + 1 < blocks else zero
    left = tile_at(ref, plane, row, block - 1) if block else zero
    return centre, (
        (tile_at(ref, plane + 1, row, block), tile_at(ref, plane - 1, row, block)),
        (
            pltpu.roll(jnp.where(r == 0, tile_at(ref, plane, above, block), centre), ROWS - 1, 0),
            pltpu.roll(jnp.where(r == ROWS - 1, tile_at(ref, plane, below, block), centre), 1, 0),
        ),
        (
            pltpu.roll(jnp.where(c == 0, right, centre), LANES - 1, 1),
            pltpu.roll(jnp.where(c == LANES - 1, left, centre), 1, 1),
        ),
    )


def stepped(e_ref, k_ref, u_ref, plane, row, blocks, block):
    row = pl.multiple_of(row, ROWS)
    above = pl.multiple_of(jnp.minimum(row + ROWS, e_ref.shape[1] - ROWS), ROWS)
    below = pl.multiple_of(jnp.maximum(row - ROWS, 0), ROWS)
    e, es = neighbours(e_ref, plane + 1, row, above, below, blocks, block)
    k, ks = neighbours(k_ref, plane + 1, row, above, below, blocks, block)
    change = None
    for d in range(3):
        (e_up, e_low), (k_up, k_low) = es[d], ks[d]
        speed = u_ref[d, plane, pl.ds(row, ROWS), block * LANES : (block + 1) * LANES]
        gain = (0.5 * (k + k_up) - jnp.minimum(speed, 0.0)) * (e_up - e)
        loss = (0.5 * (k + k_low) + jnp.maximum(speed, 0.0)) * (e - e_low)
        change = gain - loss if change is None else change + (gain - loss)
    return e + change


def gather_rows(rows, cut, window, span, me, slots, ends, e, k, u):
    begin, end = window
    quarters = len(slots)
    planes = [(lax.rem(me - s + quarters, quarters), parts, True) for s, parts in enumerate(slots)]
    for plane, parts, inside in planes + [(*pair, False) for pair in ends]:
        up = plane + 1 if inside else plane
        for field in range(5 if inside else 2):
            if field == 0 and e is None:
                continue
            for part, at, row, size in segments(
                field, rows, cut, *(window if field < 2 else span)
            ):
                to, value = pl.ds(row - begin, size), parts[part][at : at + size]
                if field < 2:
                    (e, k)[field][up, to] = value
                else:
                    u[field - 2, plane, to] = value
        if begin < 0:
            tile = parts[0][2 * cut : 2 * cut + ROWS]
            if e is not None:
                e[up, :ROWS] = down(tile, 6)
            k[up, :ROWS] = down(tile, 4)
            for d in range(3 if inside and span[0] < 0 else 0):
                u[d, plane, :ROWS] = down(tile, 3 - d)
        if end > rows:
            tile = parts[1][2 * (rows - cut) : 2 * (rows - cut) + ROWS]
            to = pl.ds(end - begin - ROWS, ROWS)
            if e is not None:
                e[up, to] = tile
            k[up, to] = down(tile, -2)
            for d in range(3 if inside and span[1] > rows else 0):
                u[d, plane, to] = down(tile, -4 - d)


def scratch(quarters, tall, width):
    return [
        pltpu.VMEM((quarters + 2, tall, width), F32),
        pltpu.VMEM((quarters + 2, tall, width), F32),
        pltpu.VMEM((3, quarters, tall, width), F32),
    ]


def grouped(refs, counts):
    out = []
    for count in counts:
        out.append(refs[:count])
        refs = refs[count:]
    return out + [refs]


def first_body(rows, cut, window, span, sent, chosen, quarters, blocks, given, idx, *refs):
    *slots, even, odd, refs = grouped(refs, [given[0]] * quarters + [given[1]] * 2)
    half, *half_ends = refs[:-3]
    e, k, u = refs[-3:]
    lowest, stride, count = chosen
    me = idx[0]
    last = end_planes(idx, quarters)
    ends = [(beyond(plane), parts) for plane, parts in zip(last, (even, odd))]
    gather_rows(rows, cut, window, span, me, slots, ends, e, k, u)
    begin = window[0]
    tiles = (span[1] - span[0]) // ROWS

    def tile_step(n, _):
        place, at = n // tiles, span[0] + (n % tiles) * ROWS
        plane = lowest + place * stride
        outside = ((at < 0) & (me == 0)) | ((at >= rows) & (me == quarters - 1))
        to = pl.ds(pl.multiple_of(at - span[0], ROWS), ROWS)
        for block in range(blocks):
            value = stepped(e, k, u, plane, at - begin, blocks, block)
            value = jnp.where(outside, 0.0, value)
            half[place, to, block * LANES : (block + 1) * LANES] = value
        return 0

    lax.fori_loop(0, count * tiles, tile_step, 0, unroll=UNROLL)
    for plane, ref in zip(last, half_ends):
        place = jnp.where(plane == 0, 0, count - 1)
        ref[...] = half[place, sent[0] - span[0] : sent[1] - span[0]]


def first_step(idx, slots, even, odd, rows, cut, window, span, sent, chosen):
    quarters, width = len(slots), even[0].shape[1]
    given = (len(slots[0]), len(even))
    flat = [x for parts in slots for x in parts] + list(even) + list(odd)
    ends = [jax.ShapeDtypeStruct((sent[1] - sent[0], width), F32)] * (2 if sent[0] < sent[1] else 0)
    return pl.pallas_call(
        functools.partial(
            first_body, rows, cut, window, span, sent, chosen, quarters, width // LANES, given
        ),
        out_shape=[jax.ShapeDtypeStruct((chosen[2], span[1] - span[0], width), F32), *ends],
        in_specs=[SMEM] + [VMEM] * len(flat),
        out_specs=[VMEM] * (1 + len(ends)),
        scratch_shapes=scratch(quarters, window[1] - window[0], width),
        compiler_params=params(),
        name="first_step",
    )(idx, *flat)


def second_body(rows, cut, window, span, quarters, blocks, given, halves, before, idx, *refs):
    *slots, even, odd, half, half_even, half_odd, early, pieces, refs = grouped(
        refs, [given[0]] * quarters + [given[1]] * 2 + [len(halves)] * 3 + [before, blocks // 2]
    )
    total_ref, e, k, u, result, totals = refs
    me, my = idx[0], idx[1]
    outer = [beyond(plane) for plane in end_planes(idx, quarters)]
    ends = list(zip(outer, (even, odd)))
    gather_rows(rows, cut, window, span, me, slots, ends, None, k, u)
    begin = window[0]
    for ref, *sides, (start, row, end, own, given) in zip(half, half_even, half_odd, halves):
        if start < end:
            for place, plane in enumerate(own):
                e[plane + 1, row - begin : end - begin] = ref[place, row - start : end - start]
        first, last = max(row, span[0]), min(end, span[1])
        if first >= last or not given:
            continue
        at = max(start, 0)
        for plane, side in zip(outer, sides):
            e[plane, first - begin : last - begin] = side[first - at : last - at]
    tiles = (span[1] - span[0]) // ROWS
    totals[...] = jnp.zeros(totals.shape, F32)

    def tile_step(n, _):
        plane, at = n // tiles, pl.multiple_of((n % tiles) * ROWS, ROWS)
        values = []
        for block in range(blocks):
            value = stepped(e, k, u, plane, at + (span[0] - begin), blocks, block)
            result[plane, pl.ds(at, ROWS), block * LANES : (block + 1) * LANES] = value
            values.append(value)
        while len(values) > 1:
            values = [a + b for a, b in zip(values[0::2], values[1::2])]
        totals[plane] = totals[plane] + values[0]
        return 0

    lax.fori_loop(0, quarters * tiles, tile_step, 0, unroll=UNROLL)
    lane = lanes_of((ROWS, LANES))
    found = jnp.zeros((ROWS, LANES), F32)
    for plane in range(quarters):
        found = jnp.where(lane == my * quarters + plane, jnp.sum(totals[plane]), found)
    for n in range(blocks):
        lanes = pl.ds(pl.multiple_of(jnp.bitwise_xor(my, n) * LANES, LANES), LANES)
        pieces[n // 2][n % 2] = result[:, :, lanes]
    if before:
        total_ref[...] = jnp.broadcast_to((early[0][...] + found)[:1], total_ref.shape)
    else:
        total_ref[...] = found


def second_step(
    idx, slots, even, odd, half, half_even, half_odd, early, rows, cut, window, span, halves, count
):
    quarters, width = len(slots), half[0].shape[2]
    given, blocks, size = (len(slots[0]), len(even)), width // LANES, span[1] - span[0]
    flat = [x for parts in slots for x in parts] + list(even) + list(odd)
    flat += list(half) + list(half_even) + list(half_odd) + list(early)
    before = len(early)
    shapes = [jax.ShapeDtypeStruct((2, quarters, size, LANES), F32)] * (blocks // 2)
    shapes += [jax.ShapeDtypeStruct((count if before else ROWS, LANES), F32)]
    out = pl.pallas_call(
        functools.partial(
            second_body, rows, cut, window, span, quarters, blocks, given, halves, before
        ),
        out_shape=shapes,
        in_specs=[SMEM] + [VMEM] * len(flat),
        out_specs=[VMEM] * len(shapes),
        scratch_shapes=scratch(quarters, window[1] - window[0], width)
        + [pltpu.VMEM((quarters, size, width), F32), pltpu.VMEM((quarters, ROWS, LANES), F32)],
        compiler_params=params(),
        name="second_step",
    )(idx, *flat)
    return out[:-1], out[-1]


def pass_on_body(counts, *refs):
    *groups, (out,) = grouped(refs, counts)
    row = 0
    for group in groups:
        size = group[0].shape[2]
        for n, pair in enumerate(group):
            out[n, :, row : row + size] = pair[1]
        row += size


def pass_on(groups):
    _, quarters, _, lanes = groups[0][0].shape
    rows = sum(group[0].shape[2] for group in groups)
    flat = [pair for group in groups for pair in group]
    return pl.pallas_call(
        functools.partial(pass_on_body, [len(group) for group in groups]),
        out_shape=jax.ShapeDtypeStruct((len(groups[0]), quarters, rows, lanes), F32),
        in_specs=[VMEM] * len(flat),
        out_specs=VMEM,
        compiler_params=params(),
        name="pass_on",
    )(*flat)


def finish_body(counts, quarters, cells, idx, found, passed, *refs):
    *groups, (out, mean, running, held, sem, held_sem) = grouped(refs, counts)
    my, pieces, row = idx[1], [], 0

    def planes_from(n):
        return pl.ds(jnp.bitwise_xor(my, n) * quarters, quarters)

    for n in range(counts[0]):
        to = out.at[planes_from(2 * n + 1)]
        pieces.append(pltpu.make_async_copy(passed.at[n], to, sem))
    for group in groups:
        size = group[0].shape[2]
        for n, pair in enumerate(group):
            to = out.at[planes_from(2 * n), pl.ds(row, size)]
            pieces.append(pltpu.make_async_copy(pair.at[0], to, sem))
        row += size
    for copy in pieces:
        copy.start()
    planes, stack = held.shape[2], idx[2]

    def stack_sum(stack):
        rows = found[pl.ds(pl.multiple_of(stack * planes, ROWS), planes)]
        tiles = [rows[n : n + ROWS] for n in range(0, planes, ROWS)]
        while len(tiles) > 1:
            tiles = [a + b for a, b in zip(tiles[0::2], tiles[1::2])]
        return tiles[0]

    here = jnp.sum(stack_sum(stack), 0, keepdims=True)
    zero = jnp.zeros((ROWS, LANES), F32)
    lower = lax.fori_loop(0, stack, lambda n, total: total + stack_sum(n), zero)
    lane = lanes_of(here.shape)
    here = here / cells
    until, by = here, 1
    while by < planes:
        until = until + jnp.where(lane >= by, pltpu.roll(until, by, 1), 0.0)
        by *= 2
    until = until + jnp.sum(lower) / cells
    rank = (stack * planes + lane + 1).astype(F32)
    held[0] = here[:, :planes]
    held[1] = (until / rank)[:, :planes]
    lines = [
        pltpu.make_async_copy(held.at[n], line, held_sem) for n, line in enumerate((mean, running))
    ]
    for copy in lines:
        copy.start()
    for copy in pieces + lines:
        copy.wait()


def finish(idx, found, passed, groups, cells):
    pairs, quarters, rows, lanes = passed.shape
    flat = [pair for group in groups for pair in group]
    counts = [len(group) for group in groups]
    planes = 2 * pairs * quarters
    line = jax.ShapeDtypeStruct((1, planes), F32)
    return pl.pallas_call(
        functools.partial(finish_body, counts, quarters, cells),
        out_shape=[jax.ShapeDtypeStruct((planes, rows, lanes), F32), line, line],
        in_specs=[SMEM, VMEM] + [ANY] * (1 + len(flat)),
        out_specs=[ANY] * 3,
        scratch_shapes=[
            pltpu.VMEM((2, 1, planes), F32),
            pltpu.SemaphoreType.DMA,
            pltpu.SemaphoreType.DMA,
        ],
        compiler_params=params(),
        name="finish",
    )(idx, found, passed, *flat)


def shift(size, by):
    return [(i, (i + by) % size) for i in range(size)]


def over_chips(pairs, sides):
    got = [pairs[0]]
    for n, pair in enumerate(pairs[1:], 1):
        where = [(i, i ^ (2 * n)) for i in range(sides)]
        got.append(lax.ppermute(pair, "gy", where))
    return got


def both_steps(energy, flow):
    quarters, sides, stacks = (lax.axis_size(a) for a in ("gx", "gy", "gz"))
    idx = jnp.stack([lax.axis_index(a) for a in ("gx", "gy", "gz")]).astype(jnp.int32)
    rows, cut = energy.shape[1] // quarters, FIRST
    done = cut - ROWS
    cells = energy.shape[1] * energy.shape[2]
    energy = pltpu.with_memory_space_constraint(energy, pltpu.HBM)
    flow = pltpu.with_memory_space_constraint(flow, pltpu.HBM)

    others = (1, *range(quarters - 1, 1, -1))
    sent = pack(idx, energy, flow, quarters, cut, others, (0,))
    later = pack(idx, energy, flow, quarters, cut, others, (1, 2))
    sent = {slot: a + b for slot, a, b in zip(others, sent, later)}
    got = {
        (slot, part): lax.ppermute(sent[slot][part], "gx", shift(quarters, slot))
        for part in range(3)
        for slot in others
    }
    own = pack(idx, energy, flow, quarters, cut, (0,), (0, 1, 2))[0]
    slots = [own] + [[got[slot, part] for part in range(3)] for slot in range(1, quarters)]
    firsts = [parts[:1] for parts in slots]

    def place_of(stack):
        stack %= stacks * sides
        return (stack % sides) * stacks + stack // sides

    def exchanged(even, odd):
        got = []
        for start, value in ((1, odd), (0, even)):
            lows = [(place_of(n), place_of(n + 1)) for n in range(start, stacks * sides, 2)]
            pairs = lows + [(b, a) for a, b in lows]
            got.append(lax.ppermute(value, ("gy", "gz"), pairs))
        return got[1], got[0]

    last = ends(idx, [s[0] for s in slots], 2 * cut + ROWS)
    even, odd = ([x] for x in exchanged(*last))
    every = tuple(range(quarters))
    args = (rows, cut, (-ROWS, cut), (-ROWS, cut), (0, done), (0, 1, quarters))
    half_a, *last = first_step(idx, firsts, even, odd, *args)
    even_a, odd_a = exchanged(*last)
    args = ([half_a], [even_a], [odd_a], (), rows, cut, (-ROWS, cut), (0, done))
    args += (((-ROWS, -ROWS, cut, every, True),), 0)
    pieces_a, sums = second_step(idx, firsts, even, odd, *args)
    pieces_a = over_chips(pieces_a, sides)

    last = ends(idx, [s[1] for s in slots], 2 * (rows - cut) + ROWS)
    even, odd = (a + [b] for a, b in zip((even, odd), exchanged(*last)))
    top = rows + ROWS
    args = (rows, cut, (done - ROWS, top), (done, top))
    outer, inner = (0, quarters - 1, 2), (1, 1, quarters - 2)
    half_b, *last = first_step(idx, slots, even, odd, *args, (done, rows), outer)
    even_b, odd_b = exchanged(*last)
    (half_c,) = first_step(idx, slots, even, odd, *args, (0, 0), inner)
    halves = [half_a, half_b, half_c], [even_a, even_b, even_b], [odd_a, odd_b, odd_b]
    args = (*halves, (sums,), rows, cut, (done - ROWS, top), (done, rows))
    args += (
        (
            (-ROWS, done - ROWS, done, every, False),
            (done, done, top, (0, quarters - 1), True),
            (done, done, top, every[1:-1], False),
        ),
    )
    args += (quarters * sides * stacks,)
    pieces_b, sums = second_step(idx, slots, even, odd, *args)
    pieces_b = over_chips(pieces_b, sides)

    everyone = functools.partial(lax.all_to_all, tiled=True)
    found = everyone(sums, ("gz", "gy", "gx"), 0, 0)
    groups = [pieces_a, pieces_b]
    passed = pass_on(groups)
    passed = lax.ppermute(passed, "gy", [(i, i ^ 1) for i in range(sides)])
    out = finish(idx, found, passed, groups, cells)
    return out[0], out[1].reshape(-1), out[2].reshape(-1)


def solution(mesh):
    placed = (P(("gz", "gy", "gx"), None, None), P(None, ("gz", "gy", "gx"), None, None))
    return jax.shard_map(
        both_steps,
        mesh=mesh,
        in_specs=placed,
        out_specs=(P("gz", "gx", "gy"), P("gz"), P("gz")),
        check_vma=False,
    )
```

```python
import functools

import jax
import jax.numpy as jnp
from jax import lax
from jax.experimental import pallas as pl
from jax.experimental.pallas import tpu as pltpu
from jax.sharding import PartitionSpec as P

F32 = jnp.float32
ANY = pl.BlockSpec(memory_space=pl.ANY)
SMEM = pl.BlockSpec(memory_space=pltpu.SMEM)
VMEM = pl.BlockSpec(memory_space=pltpu.VMEM)
HBM = pl.BlockSpec(memory_space=pltpu.HBM)
LANES = 128
ROWS = 8
FIRST = 32
UNROLL = 4


def params(mib=24):
    return pltpu.CompilerParams(vmem_limit_bytes=mib * 2**20)


def rows_of(shape):
    return lax.broadcasted_iota(jnp.int32, shape, 0)


def lanes_of(shape):
    return lax.broadcasted_iota(jnp.int32, shape, 1)


def down(tile, count):
    count %= ROWS
    return pltpu.roll(tile, count, 0) if count else tile


def part_rows(rows, cut):
    rest = rows - cut
    return (5 * cut + ROWS, 2 * rest + ROWS, 3 * rest)


def edge_row(part, rows, cut):
    return 2 * (rows - cut if part else cut)


def segments(field, rows, cut, begin, end):
    rest, found = rows - cut, []
    low, high = max(begin, 0), min(end, cut)
    if low < high:
        at = field * cut if field < 2 else field * cut + ROWS
        found.append((0, at + low, low, high - low))
    low, high = max(begin, cut), min(end, rows)
    if low < high:
        part, at = (1, field * rest) if field < 2 else (2, (field - 2) * rest)
        found.append((part, at + low - cut, low, high - low))
    return found


def pack_body(quarters, rows, cut, slots, parts, idx, energy, flow, *refs):
    count = len(slots) * len(parts)
    outs, (low, high, sem, tile_sem) = refs[:count], refs[count:]
    me = idx[0]
    fields = [energy.at[0]] + [flow.at[c, 0] for c in (3, 0, 1, 2)]
    copies, tiles = [], []
    for n, slot in enumerate(slots):
        first = pl.multiple_of(lax.rem(me + slot, quarters) * rows, ROWS)
        before = pl.multiple_of(jnp.maximum(first - ROWS, 0), ROWS)
        after = pl.multiple_of(jnp.minimum(first + rows, (quarters - 1) * rows), ROWS)
        for f, field in enumerate(fields):
            if 0 in parts:
                tiles.append(
                    pltpu.make_async_copy(field.at[pl.ds(before, ROWS)], low.at[n, f], tile_sem)
                )
            if 1 in parts:
                tiles.append(
                    pltpu.make_async_copy(field.at[pl.ds(after, ROWS)], high.at[n, f], tile_sem)
                )
    for copy in tiles:
        copy.start()
    for n, slot in enumerate(slots):
        first = lax.rem(me + slot, quarters) * rows
        for f, field in enumerate(fields):
            for part, at, row, size in segments(f, rows, cut, 0, rows):
                if part in parts:
                    out = outs[n * len(parts) + parts.index(part)]
                    source = field.at[pl.ds(pl.multiple_of(first + row, ROWS), size)]
                    copies.append(pltpu.make_async_copy(source, out.at[pl.ds(at, size)], sem))
    for copy in copies:
        copy.start()
    for copy in tiles:
        copy.wait()
    shape = low.shape[2:]
    row = rows_of(shape)
    places = ((0, 2), (2, 2), (4, 1), (5, 1), (6, 1))
    for n, slot in enumerate(slots):
        to = lax.rem(me + slot, quarters)
        for part in parts:
            if part == 2:
                continue
            tile = jnp.zeros(shape, F32)
            for f, (begin, size) in enumerate(places):
                here = (row >= begin) & (row < begin + size)
                moved = down(high[n, f], begin) if part else down(low[n, f], begin + size)
                tile = jnp.where(here, moved, tile)
            out = outs[n * len(parts) + parts.index(part)]
            at = edge_row(part, rows, cut)
            out[at : at + ROWS] = jnp.where(to == (quarters - 1 if part else 0), 0.0, tile)
    for copy in copies:
        copy.wait()


def pack(idx, energy, flow, quarters, cut, slots, parts):
    rows, width = energy.shape[1] // quarters, energy.shape[2]
    sizes = part_rows(rows, cut)
    shapes = [jax.ShapeDtypeStruct((sizes[part], width), F32) for part in parts] * len(slots)
    out = pl.pallas_call(
        functools.partial(pack_body, quarters, rows, cut, slots, parts),
        out_shape=shapes,
        in_specs=[SMEM, HBM, HBM],
        out_specs=[VMEM] * len(shapes),
        scratch_shapes=[
            pltpu.VMEM((len(slots), 5, ROWS, width), F32),
            pltpu.VMEM((len(slots), 5, ROWS, width), F32),
            pltpu.SemaphoreType.DMA,
            pltpu.SemaphoreType.DMA,
        ],
        compiler_params=params(),
        name="pack",
    )(idx, energy, flow)
    return [list(out[n * len(parts) : (n + 1) * len(parts)]) for n in range(len(slots))]


def end_planes(idx, quarters):
    above = lax.rem(idx[1], 2) == 0
    return jnp.where(above, quarters - 1, 0), jnp.where(above, 0, quarters - 1)


def beyond(plane):
    return jnp.where(plane == 0, 0, plane + 2)


def ends_body(count, idx, *refs):
    slots, outs = refs[:count], refs[count:]
    for slot, ref in enumerate(slots):
        plane = lax.rem(idx[0] - slot + count, count)
        for wanted, out in zip(end_planes(idx, count), outs):

            @pl.when(plane == wanted)
            def _():
                out[...] = ref[: out.shape[0]]


def ends(idx, slots, rows):
    shape = jax.ShapeDtypeStruct((rows, slots[0].shape[1]), F32)
    return pl.pallas_call(
        functools.partial(ends_body, len(slots)),
        out_shape=[shape] * 2,
        in_specs=[SMEM] + [VMEM] * len(slots),
        out_specs=[VMEM] * 2,
        compiler_params=params(),
        name="ends",
    )(idx, *slots)


def tile_at(ref, plane, row, block):
    return ref[plane, pl.ds(row, ROWS), block * LANES : (block + 1) * LANES]


def neighbours(ref, plane, row, above, below, blocks, block):
    centre = tile_at(ref, plane, row, block)
    r, c = rows_of(centre.shape), lanes_of(centre.shape)
    zero = jnp.zeros_like(centre)
    right = tile_at(ref, plane, row, block + 1) if block + 1 < blocks else zero
    left = tile_at(ref, plane, row, block - 1) if block else zero
    return centre, (
        (tile_at(ref, plane + 1, row, block), tile_at(ref, plane - 1, row, block)),
        (
            pltpu.roll(jnp.where(r == 0, tile_at(ref, plane, above, block), centre), ROWS - 1, 0),
            pltpu.roll(jnp.where(r == ROWS - 1, tile_at(ref, plane, below, block), centre), 1, 0),
        ),
        (
            pltpu.roll(jnp.where(c == 0, right, centre), LANES - 1, 1),
            pltpu.roll(jnp.where(c == LANES - 1, left, centre), 1, 1),
        ),
    )


def stepped(e_ref, k_ref, u_ref, plane, row, blocks, block):
    row = pl.multiple_of(row, ROWS)
    above = pl.multiple_of(jnp.minimum(row + ROWS, e_ref.shape[1] - ROWS), ROWS)
    below = pl.multiple_of(jnp.maximum(row - ROWS, 0), ROWS)
    e, es = neighbours(e_ref, plane + 1, row, above, below, blocks, block)
    k, ks = neighbours(k_ref, plane + 1, row, above, below, blocks, block)
    change = None
    for d in range(3):
        (e_up, e_low), (k_up, k_low) = es[d], ks[d]
        speed = u_ref[d, plane, pl.ds(row, ROWS), block * LANES : (block + 1) * LANES]
        gain = (0.5 * (k + k_up) - jnp.minimum(speed, 0.0)) * (e_up - e)
        loss = (0.5 * (k + k_low) + jnp.maximum(speed, 0.0)) * (e - e_low)
        change = gain - loss if change is None else change + (gain - loss)
    return e + change


def gather_rows(rows, cut, window, span, me, slots, ends, e, k, u):
    begin, end = window
    quarters = len(slots)
    planes = [(lax.rem(me - s + quarters, quarters), parts, True) for s, parts in enumerate(slots)]
    for plane, parts, inside in planes + [(*pair, False) for pair in ends]:
        up = plane + 1 if inside else plane
        for field in range(5 if inside else 2):
            if field == 0 and e is None:
                continue
            for part, at, row, size in segments(
                field, rows, cut, *(window if field < 2 else span)
            ):
                to, value = pl.ds(row - begin, size), parts[part][at : at + size]
                if field < 2:
                    (e, k)[field][up, to] = value
                else:
                    u[field - 2, plane, to] = value
        if begin < 0:
            tile = parts[0][2 * cut : 2 * cut + ROWS]
            if e is not None:
                e[up, :ROWS] = down(tile, 6)
            k[up, :ROWS] = down(tile, 4)
            for d in range(3 if inside and span[0] < 0 else 0):
                u[d, plane, :ROWS] = down(tile, 3 - d)
        if end > rows:
            tile = parts[1][2 * (rows - cut) : 2 * (rows - cut) + ROWS]
            to = pl.ds(end - begin - ROWS, ROWS)
            if e is not None:
                e[up, to] = tile
            k[up, to] = down(tile, -2)
            for d in range(3 if inside and span[1] > rows else 0):
                u[d, plane, to] = down(tile, -4 - d)


def scratch(quarters, tall, width):
    return [
        pltpu.VMEM((quarters + 2, tall, width), F32),
        pltpu.VMEM((quarters + 2, tall, width), F32),
        pltpu.VMEM((3, quarters, tall, width), F32),
    ]


def grouped(refs, counts):
    out = []
    for count in counts:
        out.append(refs[:count])
        refs = refs[count:]
    return out + [refs]


def first_body(rows, cut, window, span, sent, chosen, quarters, blocks, given, idx, *refs):
    *slots, even, odd, refs = grouped(refs, [given[0]] * quarters + [given[1]] * 2)
    half, *half_ends = refs[:-3]
    e, k, u = refs[-3:]
    lowest, stride, count = chosen
    me = idx[0]
    last = end_planes(idx, quarters)
    ends = [(beyond(plane), parts) for plane, parts in zip(last, (even, odd))]
    gather_rows(rows, cut, window, span, me, slots, ends, e, k, u)
    begin = window[0]
    tiles = (span[1] - span[0]) // ROWS

    def tile_step(n, _):
        place, at = n // tiles, span[0] + (n % tiles) * ROWS
        plane = lowest + place * stride
        outside = ((at < 0) & (me == 0)) | ((at >= rows) & (me == quarters - 1))
        to = pl.ds(pl.multiple_of(at - span[0], ROWS), ROWS)
        for block in range(blocks):
            value = stepped(e, k, u, plane, at - begin, blocks, block)
            value = jnp.where(outside, 0.0, value)
            half[place, to, block * LANES : (block + 1) * LANES] = value
        return 0

    lax.fori_loop(0, count * tiles, tile_step, 0, unroll=UNROLL)
    for plane, ref in zip(last, half_ends):
        place = jnp.where(plane == 0, 0, count - 1)
        ref[...] = half[place, sent[0] - span[0] : sent[1] - span[0]]


def first_step(idx, slots, even, odd, rows, cut, window, span, sent, chosen):
    quarters, width = len(slots), even[0].shape[1]
    given = (len(slots[0]), len(even))
    flat = [x for parts in slots for x in parts] + list(even) + list(odd)
    ends = [jax.ShapeDtypeStruct((sent[1] - sent[0], width), F32)] * (2 if sent[0] < sent[1] else 0)
    return pl.pallas_call(
        functools.partial(
            first_body, rows, cut, window, span, sent, chosen, quarters, width // LANES, given
        ),
        out_shape=[jax.ShapeDtypeStruct((chosen[2], span[1] - span[0], width), F32), *ends],
        in_specs=[SMEM] + [VMEM] * len(flat),
        out_specs=[VMEM] * (1 + len(ends)),
        scratch_shapes=scratch(quarters, window[1] - window[0], width),
        compiler_params=params(),
        name="first_step",
    )(idx, *flat)


def second_body(rows, cut, window, span, quarters, blocks, given, halves, before, idx, *refs):
    *slots, even, odd, half, half_even, half_odd, early, pieces, refs = grouped(
        refs, [given[0]] * quarters + [given[1]] * 2 + [len(halves)] * 3 + [before, blocks // 2]
    )
    total_ref, e, k, u, result, totals, *held = refs
    me, my = idx[0], idx[1]
    outer = [beyond(plane) for plane in end_planes(idx, quarters)]
    ends = list(zip(outer, (even, odd)))
    gather_rows(rows, cut, window, span, me, slots, ends, None, k, u)
    begin = window[0]
    for ref, *sides, (start, row, end, own, given) in zip(half, half_even, half_odd, halves):
        if start < end:
            for place, plane in enumerate(own):
                e[plane + 1, row - begin : end - begin] = ref[place, row - start : end - start]
        first, last = max(row, span[0]), min(end, span[1])
        if first >= last or not given:
            continue
        at = max(start, 0)
        for plane, side in zip(outer, sides):
            e[plane, first - begin : last - begin] = side[first - at : last - at]
    tiles = (span[1] - span[0]) // ROWS
    totals[...] = jnp.zeros(totals.shape, F32)

    def tile_step(n, _):
        plane, at = n // tiles, pl.multiple_of((n % tiles) * ROWS, ROWS)
        values = []
        for block in range(blocks):
            value = stepped(e, k, u, plane, at + (span[0] - begin), blocks, block)
            result[plane, pl.ds(at, ROWS), block * LANES : (block + 1) * LANES] = value
            values.append(value)
        while len(values) > 1:
            values = [a + b for a, b in zip(values[0::2], values[1::2])]
        totals[plane] = totals[plane] + values[0]
        return 0

    lax.fori_loop(0, quarters * tiles, tile_step, 0, unroll=UNROLL)
    lane = lanes_of((ROWS, LANES))
    found = jnp.zeros((ROWS, LANES), F32)
    for plane in range(quarters):
        found = jnp.where(lane == my * quarters + plane, jnp.sum(totals[plane]), found)
    if before:
        held, sem = held
        held[...] = jnp.broadcast_to((early[0][...] + found)[:1], held.shape)
        sending = pltpu.make_async_copy(held, total_ref, sem)
        sending.start()
    else:
        total_ref[...] = found
    for n in range(blocks):
        lanes = pl.ds(pl.multiple_of(jnp.bitwise_xor(my, n) * LANES, LANES), LANES)
        pieces[n // 2][n % 2] = result[:, :, lanes]
    if before:
        sending.wait()


def second_step(
    idx, slots, even, odd, half, half_even, half_odd, early, rows, cut, window, span, halves, count
):
    quarters, width = len(slots), half[0].shape[2]
    given, blocks, size = (len(slots[0]), len(even)), width // LANES, span[1] - span[0]
    flat = [x for parts in slots for x in parts] + list(even) + list(odd)
    flat += list(half) + list(half_even) + list(half_odd) + list(early)
    before = len(early)
    shapes = [jax.ShapeDtypeStruct((2, quarters, size, LANES), F32)] * (blocks // 2)
    shapes += [jax.ShapeDtypeStruct((count if before else ROWS, LANES), F32)]
    out = pl.pallas_call(
        functools.partial(
            second_body, rows, cut, window, span, quarters, blocks, given, halves, before
        ),
        out_shape=shapes,
        in_specs=[SMEM] + [VMEM] * len(flat),
        out_specs=[VMEM] * (len(shapes) - 1) + [ANY if before else VMEM],
        scratch_shapes=scratch(quarters, window[1] - window[0], width)
        + [pltpu.VMEM((quarters, size, width), F32), pltpu.VMEM((quarters, ROWS, LANES), F32)]
        + ([pltpu.VMEM((count, LANES), F32), pltpu.SemaphoreType.DMA] if before else []),
        compiler_params=params(),
        name="second_step",
    )(idx, *flat)
    return out[:-1], out[-1]


def pass_on_body(counts, *refs):
    *groups, (out,) = grouped(refs, counts)
    row = 0
    for group in groups:
        size = group[0].shape[2]
        for n, pair in enumerate(group):
            out[n, :, row : row + size] = pair[1]
        row += size


def pass_on(groups):
    _, quarters, _, lanes = groups[0][0].shape
    rows = sum(group[0].shape[2] for group in groups)
    flat = [pair for group in groups for pair in group]
    return pl.pallas_call(
        functools.partial(pass_on_body, [len(group) for group in groups]),
        out_shape=jax.ShapeDtypeStruct((len(groups[0]), quarters, rows, lanes), F32),
        in_specs=[VMEM] * len(flat),
        out_specs=VMEM,
        compiler_params=params(),
        name="pass_on",
    )(*flat)


def finish_body(counts, quarters, cells, idx, found, passed, *refs):
    *groups, (out, mean, running, held, sem, held_sem) = grouped(refs, counts)
    my, pieces, row = idx[1], [], 0

    def planes_from(n):
        return pl.ds(jnp.bitwise_xor(my, n) * quarters, quarters)

    for n in range(counts[0]):
        to = out.at[planes_from(2 * n + 1)]
        pieces.append(pltpu.make_async_copy(passed.at[n], to, sem))
    for group in groups:
        size = group[0].shape[2]
        for n, pair in enumerate(group):
            to = out.at[planes_from(2 * n), pl.ds(row, size)]
            pieces.append(pltpu.make_async_copy(pair.at[0], to, sem))
        row += size
    for copy in pieces:
        copy.start()
    planes, stack = held.shape[2], idx[2]

    def stack_sum(stack):
        rows = found[pl.ds(pl.multiple_of(stack * planes, ROWS), planes)]
        tiles = [rows[n : n + ROWS] for n in range(0, planes, ROWS)]
        while len(tiles) > 1:
            tiles = [a + b for a, b in zip(tiles[0::2], tiles[1::2])]
        return tiles[0]

    here = jnp.sum(stack_sum(stack), 0, keepdims=True)
    zero = jnp.zeros((ROWS, LANES), F32)
    lower = lax.fori_loop(0, stack, lambda n, total: total + stack_sum(n), zero)
    lane = lanes_of(here.shape)
    here = here / cells
    until, by = here, 1
    while by < planes:
        until = until + jnp.where(lane >= by, pltpu.roll(until, by, 1), 0.0)
        by *= 2
    until = until + jnp.sum(lower) / cells
    rank = (stack * planes + lane + 1).astype(F32)
    held[0] = here[:, :planes]
    held[1] = (until / rank)[:, :planes]
    lines = [
        pltpu.make_async_copy(held.at[n], line, held_sem) for n, line in enumerate((mean, running))
    ]
    for copy in lines:
        copy.start()
    for copy in pieces + lines:
        copy.wait()


def finish(idx, found, passed, groups, cells):
    pairs, quarters, rows, lanes = passed.shape
    flat = [pair for group in groups for pair in group]
    counts = [len(group) for group in groups]
    planes = 2 * pairs * quarters
    line = jax.ShapeDtypeStruct((1, planes), F32)
    return pl.pallas_call(
        functools.partial(finish_body, counts, quarters, cells),
        out_shape=[jax.ShapeDtypeStruct((planes, rows, lanes), F32), line, line],
        in_specs=[SMEM, VMEM] + [ANY] * (1 + len(flat)),
        out_specs=[ANY] * 3,
        scratch_shapes=[
            pltpu.VMEM((2, 1, planes), F32),
            pltpu.SemaphoreType.DMA,
            pltpu.SemaphoreType.DMA,
        ],
        compiler_params=params(),
        name="finish",
    )(idx, found, passed, *flat)


def shift(size, by):
    return [(i, (i + by) % size) for i in range(size)]


def over_chips(pairs, sides):
    got = [pairs[0]]
    for n, pair in enumerate(pairs[1:], 1):
        where = [(i, i ^ (2 * n)) for i in range(sides)]
        got.append(lax.ppermute(pair, "gy", where))
    return got


def both_steps(energy, flow):
    quarters, sides, stacks = (lax.axis_size(a) for a in ("gx", "gy", "gz"))
    idx = jnp.stack([lax.axis_index(a) for a in ("gx", "gy", "gz")]).astype(jnp.int32)
    rows, cut = energy.shape[1] // quarters, FIRST
    done = cut - ROWS
    cells = energy.shape[1] * energy.shape[2]
    energy = pltpu.with_memory_space_constraint(energy, pltpu.HBM)
    flow = pltpu.with_memory_space_constraint(flow, pltpu.HBM)

    others = (1, *range(quarters - 1, 1, -1))
    sent = pack(idx, energy, flow, quarters, cut, others, (0,))
    later = pack(idx, energy, flow, quarters, cut, others, (1, 2))
    sent = {slot: a + b for slot, a, b in zip(others, sent, later)}
    got = {
        (slot, part): lax.ppermute(sent[slot][part], "gx", shift(quarters, slot))
        for part in range(3)
        for slot in others
    }
    own = pack(idx, energy, flow, quarters, cut, (0,), (0, 1, 2))[0]
    slots = [own] + [[got[slot, part] for part in range(3)] for slot in range(1, quarters)]
    firsts = [parts[:1] for parts in slots]

    def place_of(stack):
        stack %= stacks * sides
        return (stack % sides) * stacks + stack // sides

    def exchanged(even, odd):
        got = []
        for start, value in ((1, odd), (0, even)):
            lows = [(place_of(n), place_of(n + 1)) for n in range(start, stacks * sides, 2)]
            pairs = lows + [(b, a) for a, b in lows]
            got.append(lax.ppermute(value, ("gy", "gz"), pairs))
        return got[1], got[0]

    last = ends(idx, [s[0] for s in slots], 2 * cut + ROWS)
    even, odd = ([x] for x in exchanged(*last))
    every = tuple(range(quarters))
    args = (rows, cut, (-ROWS, cut), (-ROWS, cut), (0, done), (0, 1, quarters))
    half_a, *last = first_step(idx, firsts, even, odd, *args)
    even_a, odd_a = exchanged(*last)
    args = ([half_a], [even_a], [odd_a], (), rows, cut, (-ROWS, cut), (0, done))
    args += (((-ROWS, -ROWS, cut, every, True),), 0)
    pieces_a, sums = second_step(idx, firsts, even, odd, *args)
    pieces_a = over_chips(pieces_a, sides)

    last = ends(idx, [s[1] for s in slots], 2 * (rows - cut) + ROWS)
    even, odd = (a + [b] for a, b in zip((even, odd), exchanged(*last)))
    top = rows + ROWS
    args = (rows, cut, (done - ROWS, top), (done, top))
    outer, inner = (0, quarters - 1, 2), (1, 1, quarters - 2)
    half_b, *last = first_step(idx, slots, even, odd, *args, (done, rows), outer)
    even_b, odd_b = exchanged(*last)
    (half_c,) = first_step(idx, slots, even, odd, *args, (0, 0), inner)
    halves = [half_a, half_b, half_c], [even_a, even_b, even_b], [odd_a, odd_b, odd_b]
    args = (*halves, (sums,), rows, cut, (done - ROWS, top), (done, rows))
    args += (
        (
            (-ROWS, done - ROWS, done, every, False),
            (done, done, top, (0, quarters - 1), True),
            (done, done, top, every[1:-1], False),
        ),
    )
    args += (quarters * sides * stacks,)
    pieces_b, sums = second_step(idx, slots, even, odd, *args)
    pieces_b = over_chips(pieces_b, sides)

    everyone = functools.partial(lax.all_to_all, tiled=True)
    found = everyone(sums, ("gz", "gy", "gx"), 0, 0)
    groups = [pieces_a, pieces_b]
    passed = pass_on(groups)
    passed = lax.ppermute(passed, "gy", [(i, i ^ 1) for i in range(sides)])
    out = finish(idx, found, passed, groups, cells)
    return out[0], out[1].reshape(-1), out[2].reshape(-1)


def solution(mesh):
    placed = (P(("gz", "gy", "gx"), None, None), P(None, ("gz", "gy", "gx"), None, None))
    return jax.shard_map(
        both_steps,
        mesh=mesh,
        in_specs=placed,
        out_specs=(P("gz", "gx", "gy"), P("gz"), P("gz")),
        check_vma=False,
    )
```
